8 devices in a mesh: dp: 1 (over z), sp: 8 (over x, y, core).
Axes of the slice: x: 2, y: 2, z: 1, core: 2. Of those that a mesh axis runs over, the one named last changes fastest.
Arguments:
- q: bfloat16 [32, 32, 128], P('dp')
- k: bfloat16 [32, 8192, 4, 128], P('dp', 'sp')
- v: bfloat16 [32, 8192, 4, 128], P('dp', 'sp')
Outputs:
- q: bfloat16 [32, 32, 128], P('dp')
All inputs are finite; a program needn't handle non-finite values.
Results may differ from the reference program's by a relative error of at most 0.012.
Values are sent between devices in bfloat16 or wider.
A program may use at most 2 GiB of HBM per device.

```python
import jax
import jax.numpy as jnp

BATCH = 32
CACHE = 8192
HEADS = 32
KV_HEADS = 4
HEAD = 128


def setup_inputs(seed: int = 0, part: int = 0) -> dict:
    kq, kk, kv = (jax.random.fold_in(k, part) for k in jax.random.split(jax.random.key(seed), 3))
    return {
        "q": (3 * jax.random.normal(kq, (BATCH, HEADS, HEAD), jnp.float32)).astype(jnp.bfloat16),
        "k": jax.random.normal(kk, (BATCH, CACHE, KV_HEADS, HEAD), jnp.float32).astype(jnp.bfloat16),
        "v": jax.random.normal(kv, (BATCH, CACHE, KV_HEADS, HEAD), jnp.float32).astype(jnp.bfloat16),
    }


def einsum(form, a, b):
    return jnp.einsum(form, a.astype(jnp.float32), b.astype(jnp.float32))


def reference(q, k, v):
    grouped = q.reshape(BATCH, KV_HEADS, -1, HEAD)
    scores = einsum("bgsd,bugd->bgsu", grouped, k) * HEAD**-0.5
    weights = jax.nn.softmax(scores, -1).astype(jnp.bfloat16)
    return einsum("bgsu,bugd->bgsd", weights, v).astype(jnp.bfloat16).reshape(BATCH, HEADS, HEAD)
```

```python
import functools

import jax
import jax.numpy as jnp
from jax import lax
from jax.experimental import pallas as pl
from jax.experimental.pallas import tpu as pltpu
from jax.sharding import PartitionSpec as P

LOG2E = 1.4426950408889634
TILE = 256
TAIL = 2
LAG = 3
K_SLOTS, V_SLOTS = 4, 5


def spread(x, reduce, fill, kinds):
    lane = lax.broadcasted_iota(jnp.int32, x.shape, 1) % kinds
    out = None
    for g in range(kinds):
        one = jnp.broadcast_to(reduce(jnp.where(lane == g, x, fill), axis=1, keepdims=True), x.shape)
        out = one if out is None else jnp.where(lane == g, one, out)
    return out


def columns(x):
    return [x[:, i : i + 128] for i in range(0, x.shape[1], 128)]


def weigh(q, keys, held, scale):
    half = keys.shape[0] // 2
    none = jnp.zeros_like(q)
    both = jnp.concatenate([jnp.concatenate([q, none], 1), jnp.concatenate([none, q], 1)], 0)
    lane = lax.broadcasted_iota(jnp.int32, (8, TILE), 1) % 4
    tiles = []
    for j in range(0, half, TILE):
        pair = jnp.concatenate([keys[j : j + TILE, :], keys[half + j : half + j + TILE, :]], 1)
        scores = lax.dot_general(both, pair, (((1,), (1,)), ((), ())), preferred_element_type=jnp.float32)
        for a in (0, 32):
            own = scores[a : a + 8]
            for g in range(1, 4):
                own = jnp.where(lane == g, scores[a + 8 * g : a + 8 * g + 8], own)
            tiles.append(own)
    high = spread(functools.reduce(jnp.maximum, columns(functools.reduce(jnp.maximum, tiles))), jnp.max, -jnp.inf, 4)
    wide = jnp.concatenate([high] * (TILE // 128), 1)
    total = None
    for j in range(half // TILE):
        rows = []
        for own in tiles[2 * j : 2 * j + 2]:
            weights = jnp.exp2((own - wide) * scale)
            total = weights if total is None else total + weights
            rows += [jnp.where(lane == g, weights, 0.0) for g in range(4)]
        held[:, j * TILE : (j + 1) * TILE] = jnp.concatenate(rows, 0).astype(jnp.bfloat16)
    return high, spread(functools.reduce(jnp.add, columns(total)), jnp.sum, 0.0, 4)


def gather(held, values):
    half = values.shape[0] // 2
    out = None
    for r in range(0, half, half // 2):
        rows = jnp.concatenate([values[r : r + half // 2, :], values[half + r : half + r + half // 2, :]], 1)
        seen = jnp.dot(held[:, r : r + half // 2], rows, preferred_element_type=jnp.float32)
        seen = seen[0:32, 0:128] + seen[32:64, 128:256]
        out = seen if out is None else out + seen
    return out


def kernel(n, q, k, v, out, kbuf, vbuf, held0, held1, part, stat, parts, stats, ksem, vsem, sent, told, came, passed, landed):
    me = lax.axis_index("sp")
    pairs = q.shape[0] // 2
    bulk = pairs - TAIL
    rounds = -(-bulk // n)
    scale = q.shape[2] ** -0.5 * LOG2E
    held = (held0, held1)

    def read(src, buf, sem, slots, i):
        slot = lax.rem(i, slots)
        return pltpu.make_async_copy(src.at[pl.ds(2 * i, 2)], buf.at[slot], sem.at[slot])

    read_k = functools.partial(read, k, kbuf, ksem, K_SLOTS)
    read_v = functools.partial(read, v, vbuf, vsem, V_SLOTS)
    for i in range(max(K_SLOTS, V_SLOTS)):
        if i < K_SLOTS:
            read_k(i).start()
        if i < V_SLOTS:
            read_v(i).start()

    barrier = pltpu.get_barrier_semaphore()
    for d in range(1, n):
        pl.semaphore_signal(barrier, inc=1, device_id={"sp": lax.rem(me + d, n)}, device_id_type=pl.DeviceIdType.MESH)

    def keys(i):
        slot = lax.rem(i, K_SLOTS)
        lane = lax.broadcasted_iota(jnp.int32, (8, 128), 1)
        found = [weigh(q[2 * i + u], kbuf.at[slot, u], held[u], scale) for u in range(2)]
        stat[i] = jnp.where(lane < 64, jnp.where(lane < 32, *found[0]), jnp.where(lane < 96, *found[1]))

    def values(i):
        slot = lax.rem(i, V_SLOTS)
        for u in range(2):
            part[i, u] = gather(held[u], vbuf.at[slot, u]).astype(jnp.bfloat16)

    def send(i, place, to, sems):
        return [
            pltpu.make_async_remote_copy(
                src_ref=src.at[i], dst_ref=dst.at[place, me], send_sem=sems.at[kind], recv_sem=came.at[place, me, kind], device_id={"sp": to}, device_id_type=pl.DeviceIdType.MESH
            )
            for kind, (src, dst) in enumerate(((part, parts), (stat, stats)))
        ]

    def keep(i, place):
        parts[place, me] = part[i]
        stats[place, me] = stat[i]

    def to_owner(i):
        return send(i, i // n, lax.rem(i, n), sent.at[i])

    def to_all(i, d):
        return send(i, rounds + i - bulk, lax.rem(me + d, n), told.at[i - bulk, d - 1])

    def share(i):
        @pl.when(i < bulk)
        def _():
            @pl.when(lax.rem(i, n) == me)
            def _():
                keep(i, i // n)

            @pl.when(lax.rem(i, n) != me)
            def _():
                for copy in to_owner(i):
                    copy.start()

        @pl.when(i >= bulk)
        def _():
            for d in range(1, n):
                for copy in to_all(i, d):
                    copy.start()
            keep(i, rounds + i - bulk)

    def together(i, place):
        for d in range(1, n):
            other = lax.rem(me + d, n)
            for kind, dst in enumerate((parts, stats)):
                pltpu.make_async_remote_copy(
                    src_ref=dst.at[place, other], dst_ref=dst.at[place, other], send_sem=came.at[place, other, kind], recv_sem=came.at[place, other, kind],
                    device_id={"sp": other}, device_id_type=pl.DeviceIdType.MESH,
                ).wait_recv()
        for u in range(2):
            result = []
            for g in range(4):
                high, total = ([jnp.broadcast_to(stats[place, p][:, at : at + 1], (8, 128)) for p in range(n)] for at in (64 * u + g, 64 * u + 32 + g))
                top = functools.reduce(jnp.maximum, high)
                by = [jnp.exp2((h - top) * scale) for h in high]
                whole = functools.reduce(jnp.add, [w * t for w, t in zip(by, total)])
                seen = functools.reduce(jnp.add, [w * parts[place, p, u, 8 * g : 8 * g + 8, :].astype(jnp.float32) for p, w in enumerate(by)])
                result.append(seen / whole)
            out[2 * i + u] = jnp.concatenate(result, 0).astype(out.dtype)

    def announce(i, d):
        here = out.at[pl.ds(2 * i, 2)]
        return pltpu.make_async_remote_copy(
            src_ref=here, dst_ref=here, send_sem=passed.at[i // n, d - 1], recv_sem=landed.at[i], device_id={"sp": lax.rem(me + d, n)}, device_id_type=pl.DeviceIdType.MESH
        )

    def own(i):
        @pl.when((i >= 0) & (i < bulk) & (lax.rem(i + n, n) == me))
        def _():
            together(i, i // n)
            for d in range(1, n):
                announce(i, d).start()

    read_k(0).wait()
    keys(0)
    read_k(K_SLOTS).start()
    pl.semaphore_wait(barrier, n - 1)

    def step(i, _):
        read_v(i - 1).wait()
        read_k(i).wait()
        values(i - 1)
        keys(i)

        @pl.when(i + K_SLOTS < pairs)
        def _():
            read_k(i + K_SLOTS).start()

        @pl.when(i - 1 + V_SLOTS < pairs)
        def _():
            read_v(i - 1 + V_SLOTS).start()

        share(i - 1)
        own(i - 1 - LAG)
        return 0

    lax.fori_loop(1, pairs, step, 0)
    read_v(pairs - 1).wait()
    values(pairs - 1)
    share(jnp.int32(pairs - 1))

    def rest(i, _):
        own(i)
        return 0

    lax.fori_loop(pairs - 1 - LAG, bulk, rest, 0)

    def last(i, _):
        together(i, rounds + i - bulk)
        return 0

    lax.fori_loop(bulk, pairs, last, 0)

    def settle(i, _):
        @pl.when(lax.rem(i, n) != me)
        def _():
            announce(i, 1).wait_recv()
            for copy in to_owner(i):
                copy.wait_send()

        @pl.when(lax.rem(i, n) == me)
        def _():
            for d in range(1, n):
                announce(i, d).wait_send()

        return 0

    lax.fori_loop(0, bulk, settle, 0)
    for i in range(bulk, pairs):
        for d in range(1, n):
            for copy in to_all(i, d):
                copy.wait_send()


def solution(mesh):
    n = mesh.shape["sp"]

    def step(q, k, v):
        batch, heads, head = q.shape
        pairs, rows = batch // 2, k.shape[1] * k.shape[2]
        places = -(-(pairs - TAIL) // n) + TAIL
        dma = pltpu.SemaphoreType.DMA
        return pl.pallas_call(
            functools.partial(kernel, n),
            out_shape=jax.ShapeDtypeStruct(q.shape, q.dtype),
            in_specs=[pl.BlockSpec(memory_space=pltpu.VMEM), pl.BlockSpec(memory_space=pl.ANY), pl.BlockSpec(memory_space=pl.ANY)],
            out_specs=pl.BlockSpec(memory_space=pltpu.VMEM),
            scratch_shapes=[
                pltpu.VMEM((K_SLOTS, 2, rows, head), k.dtype),
                pltpu.VMEM((V_SLOTS, 2, rows, head), v.dtype),
                pltpu.VMEM((2 * heads, rows // 2), jnp.bfloat16),
                pltpu.VMEM((2 * heads, rows // 2), jnp.bfloat16),
                pltpu.VMEM((pairs, 2, heads, head), jnp.bfloat16),
                pltpu.VMEM((pairs, 8, 128), jnp.float32),
                pltpu.VMEM((places, n, 2, heads, head), jnp.bfloat16),
                pltpu.VMEM((places, n, 8, 128), jnp.float32),
                dma((K_SLOTS,)),
                dma((V_SLOTS,)),
                dma((pairs - TAIL, 2)),
                dma((TAIL, n - 1, 2)),
                dma((places, n, 2)),
                dma((places - TAIL, n - 1)),
                dma((pairs - TAIL,)),
            ],
            compiler_params=pltpu.CompilerParams(collective_id=0, has_side_effects=True, vmem_limit_bytes=40 * 1024 * 1024),
        )(q, k.reshape(batch, rows, head), v.reshape(batch, rows, head))

    return jax.shard_map(
        step,
        mesh=mesh,
        in_specs=(P("dp", None, None), P("dp", "sp", None, None), P("dp", "sp", None, None)),
        out_specs=P("dp", None, None),
        check_vma=False,
    )
```

```python
import functools

import jax
import jax.numpy as jnp
from jax import lax
from jax.experimental import pallas as pl
from jax.experimental.pallas import tpu as pltpu
from jax.sharding import PartitionSpec as P

LOG2E = 1.4426950408889634
TILE = 256
TAIL = 2
LAG = 3
K_SLOTS, V_SLOTS = 5, 6


def spread(x, reduce, fill, kinds):
    lane = lax.broadcasted_iota(jnp.int32, x.shape, 1) % kinds
    out = None
    for g in range(kinds):
        one = jnp.broadcast_to(reduce(jnp.where(lane == g, x, fill), axis=1, keepdims=True), x.shape)
        out = one if out is None else jnp.where(lane == g, one, out)
    return out


def columns(x):
    return [x[:, i : i + 128] for i in range(0, x.shape[1], 128)]


def weigh(q, keys, held, scale):
    half = keys.shape[0] // 2
    none = jnp.zeros_like(q)
    both = jnp.concatenate([jnp.concatenate([q, none], 1), jnp.concatenate([none, q], 1)], 0)
    lane = lax.broadcasted_iota(jnp.int32, (8, TILE), 1) % 4
    tiles = []
    for j in range(0, half, TILE):
        pair = jnp.concatenate([keys[j : j + TILE, :], keys[half + j : half + j + TILE, :]], 1)
        scores = lax.dot_general(both, pair, (((1,), (1,)), ((), ())), preferred_element_type=jnp.float32)
        for a in (0, 32):
            own = scores[a : a + 8]
            for g in range(1, 4):
                own = jnp.where(lane == g, scores[a + 8 * g : a + 8 * g + 8], own)
            tiles.append(own)
    high = spread(functools.reduce(jnp.maximum, columns(functools.reduce(jnp.maximum, tiles))), jnp.max, -jnp.inf, 4)
    wide = jnp.concatenate([high] * (TILE // 128), 1)
    total = None
    for j in range(half // TILE):
        rows = []
        for own in tiles[2 * j : 2 * j + 2]:
            weights = jnp.exp2((own - wide) * scale)
            total = weights if total is None else total + weights
            rows += [jnp.where(lane == g, weights, 0.0) for g in range(4)]
        held[:, j * TILE : (j + 1) * TILE] = jnp.concatenate(rows, 0).astype(jnp.bfloat16)
    return high, functools.reduce(jnp.add, columns(total))


def gather(held, values):
    half = values.shape[0] // 2
    out = None
    for r in range(0, half, half // 2):
        rows = jnp.concatenate([values[r : r + half // 2, :], values[half + r : half + r + half // 2, :]], 1)
        seen = jnp.dot(held[:, r : r + half // 2], rows, preferred_element_type=jnp.float32)
        seen = seen[0:32, 0:128] + seen[32:64, 128:256]
        out = seen if out is None else out + seen
    return out


def kernel(n, q, k, v, out, qbuf, kbuf, vbuf, held0, held1, high, sums, part, stat, parts, stats, qsem, ksem, vsem, sent, told, came, passed, landed):
    me = lax.axis_index("sp")
    pairs = q.shape[0] // 2
    bulk = pairs - TAIL
    rounds = -(-bulk // n)
    scale = q.shape[2] ** -0.5 * LOG2E
    held = (held0, held1)

    def read(src, buf, sem, slots, i):
        slot = lax.rem(i, slots)
        return pltpu.make_async_copy(src.at[pl.ds(2 * i, 2)], buf.at[slot], sem.at[slot])

    read_k = functools.partial(read, k, kbuf, ksem, K_SLOTS)
    read_v = functools.partial(read, v, vbuf, vsem, V_SLOTS)
    read_q = pltpu.make_async_copy(q, qbuf, qsem)
    read_q.start()
    for i in range(max(K_SLOTS, V_SLOTS)):
        if i < K_SLOTS:
            read_k(i).start()
        if i < V_SLOTS:
            read_v(i).start()

    barrier = pltpu.get_barrier_semaphore()
    for d in range(1, n):
        pl.semaphore_signal(barrier, inc=1, device_id={"sp": lax.rem(me + d, n)}, device_id_type=pl.DeviceIdType.MESH)

    def keys(i, u):
        high[u], sums[u] = weigh(qbuf[2 * i + u], kbuf.at[lax.rem(i, K_SLOTS), u], held[u], scale)

    def values(i, u):
        lane = lax.broadcasted_iota(jnp.int32, (8, 128), 1)
        found = jnp.where(lane % 64 < 32, high[u], spread(sums[u], jnp.sum, 0.0, 4))
        stat[i] = found if u == 0 else jnp.where(lane < 64, stat[i], found)
        part[i, u] = gather(held[u], vbuf.at[lax.rem(i, V_SLOTS), u]).astype(jnp.bfloat16)

    def send(i, place, to, sems):
        return [
            pltpu.make_async_remote_copy(
                src_ref=src.at[i], dst_ref=dst.at[place, me], send_sem=sems.at[kind], recv_sem=came.at[place, me, kind], device_id={"sp": to}, device_id_type=pl.DeviceIdType.MESH
            )
            for kind, (src, dst) in enumerate(((part, parts), (stat, stats)))
        ]

    def keep(i, place):
        parts[place, me] = part[i]
        stats[place, me] = stat[i]

    def to_owner(i):
        return send(i, i // n, lax.rem(i, n), sent.at[i])

    def to_all(i, d):
        return send(i, rounds + i - bulk, lax.rem(me + d, n), told.at[i - bulk, d - 1])

    def share(i):
        @pl.when(i < bulk)
        def _():
            @pl.when(lax.rem(i, n) == me)
            def _():
                keep(i, i // n)

            @pl.when(lax.rem(i, n) != me)
            def _():
                for copy in to_owner(i):
                    copy.start()

        @pl.when(i >= bulk)
        def _():
            for d in range(1, n):
                for copy in to_all(i, d):
                    copy.start()
            keep(i, rounds + i - bulk)

    def together(i, place):
        for d in range(1, n):
            other = lax.rem(me + d, n)
            for kind, dst in enumerate((parts, stats)):
                pltpu.make_async_remote_copy(
                    src_ref=dst.at[place, other], dst_ref=dst.at[place, other], send_sem=came.at[place, other, kind], recv_sem=came.at[place, other, kind],
                    device_id={"sp": other}, device_id_type=pl.DeviceIdType.MESH,
                ).wait_recv()
        for u in range(2):
            result = []
            for g in range(4):
                high, total = ([jnp.broadcast_to(stats[place, p][:, at : at + 1], (8, 128)) for p in range(n)] for at in (64 * u + g, 64 * u + 32 + g))
                top = functools.reduce(jnp.maximum, high)
                by = [jnp.exp2((h - top) * scale) for h in high]
                whole = functools.reduce(jnp.add, [w * t for w, t in zip(by, total)])
                seen = functools.reduce(jnp.add, [w * parts[place, p, u, 8 * g : 8 * g + 8, :].astype(jnp.float32) for p, w in enumerate(by)])
                result.append(seen / whole)
            out[2 * i + u] = jnp.concatenate(result, 0).astype(out.dtype)

    def announce(i, d):
        here = out.at[pl.ds(2 * i, 2)]
        return pltpu.make_async_remote_copy(
            src_ref=here, dst_ref=here, send_sem=passed.at[i // n, d - 1], recv_sem=landed.at[i], device_id={"sp": lax.rem(me + d, n)}, device_id_type=pl.DeviceIdType.MESH
        )

    def own(i):
        @pl.when((i >= 0) & (i < bulk) & (lax.rem(i + n, n) == me))
        def _():
            together(i, i // n)
            for d in range(1, n):
                announce(i, d).start()

    read_q.wait()
    read_k(0).wait()
    keys(0, 0)
    keys(0, 1)
    read_k(K_SLOTS).start()
    read_v(0).wait()
    values(0, 0)
    pl.semaphore_wait(barrier, n - 1)

    def step(i, _):
        read_k(i).wait()
        read_v(i).wait()
        keys(i, 0)
        values(i - 1, 1)
        keys(i, 1)
        values(i, 0)

        @pl.when(i + K_SLOTS < pairs)
        def _():
            read_k(i + K_SLOTS).start()

        @pl.when(i - 1 + V_SLOTS < pairs)
        def _():
            read_v(i - 1 + V_SLOTS).start()

        share(i - 1)
        own(i - 1 - LAG)
        return 0

    end = pairs - 1
    lax.fori_loop(1, end, step, 0)
    read_k(end).wait()
    keys(end, 0)
    values(end - 1, 1)
    share(jnp.int32(end - 1))
    keys(end, 1)
    read_v(end).wait()
    values(end, 0)
    values(end, 1)
    share(jnp.int32(end))

    def rest(i, _):
        own(i)
        return 0

    lax.fori_loop(end - 1 - LAG, bulk, rest, 0)

    def last(i, _):
        together(i, rounds + i - bulk)
        return 0

    lax.fori_loop(bulk, pairs, last, 0)

    def settle(i, _):
        @pl.when(lax.rem(i, n) != me)
        def _():
            announce(i, 1).wait_recv()
            for copy in to_owner(i):
                copy.wait_send()

        @pl.when(lax.rem(i, n) == me)
        def _():
            for d in range(1, n):
                announce(i, d).wait_send()

        return 0

    lax.fori_loop(0, bulk, settle, 0)
    for i in range(bulk, pairs):
        for d in range(1, n):
            for copy in to_all(i, d):
                copy.wait_send()


def solution(mesh):
    n = mesh.shape["sp"]

    def step(q, k, v):
        batch, heads, head = q.shape
        pairs, rows = batch // 2, k.shape[1] * k.shape[2]
        places = -(-(pairs - TAIL) // n) + TAIL
        dma = pltpu.SemaphoreType.DMA
        return pl.pallas_call(
            functools.partial(kernel, n),
            out_shape=jax.ShapeDtypeStruct(q.shape, q.dtype),
            in_specs=[pl.BlockSpec(memory_space=pltpu.HBM)] * 3,
            out_specs=pl.BlockSpec(memory_space=pltpu.VMEM),
            scratch_shapes=[
                pltpu.VMEM(q.shape, q.dtype),
                pltpu.VMEM((K_SLOTS, 2, rows, head), k.dtype),
                pltpu.VMEM((V_SLOTS, 2, rows, head), v.dtype),
                pltpu.VMEM((2 * heads, rows // 2), jnp.bfloat16),
                pltpu.VMEM((2 * heads, rows // 2), jnp.bfloat16),
                pltpu.VMEM((2, 8, 128), jnp.float32),
                pltpu.VMEM((2, 8, 128), jnp.float32),
                pltpu.VMEM((pairs, 2, heads, head), jnp.bfloat16),
                pltpu.VMEM((pairs, 8, 128), jnp.float32),
                pltpu.VMEM((places, n, 2, heads, head), jnp.bfloat16),
                pltpu.VMEM((places, n, 8, 128), jnp.float32),
                dma,
                dma((K_SLOTS,)),
                dma((V_SLOTS,)),
                dma((pairs - TAIL, 2)),
                dma((TAIL, n - 1, 2)),
                dma((places, n, 2)),
                dma((places - TAIL, n - 1)),
                dma((pairs - TAIL,)),
            ],
            compiler_params=pltpu.CompilerParams(collective_id=0, has_side_effects=True, vmem_limit_bytes=48 * 1024 * 1024),
        )(q, k.reshape(batch, rows, head), v.reshape(batch, rows, head))

    return jax.shard_map(
        step,
        mesh=mesh,
        in_specs=(P("dp", None, None), P("dp", "sp", None, None), P("dp", "sp", None, None)),
        out_specs=P("dp", None, None),
        check_vma=False,
    )
```

```python
import functools

import jax
import jax.numpy as jnp
from jax import lax
from jax.experimental import pallas as pl
from jax.experimental.pallas import tpu as pltpu
from jax.sharding import PartitionSpec as P

LOG2E = 1.4426950408889634
TILE = 256
TAIL = 3
LAG = 4
K_SLOTS, V_SLOTS = 4, 5


def spread(x, reduce, fill, kinds):
    lane = lax.broadcasted_iota(jnp.int32, x.shape, 1) % kinds
    out = None
    for g in range(kinds):
        one = jnp.broadcast_to(reduce(jnp.where(lane == g, x, fill), axis=1, keepdims=True), x.shape)
        out = one if out is None else jnp.where(lane == g, one, out)
    return out


def columns(x):
    return [x[:, i : i + 128] for i in range(0, x.shape[1], 128)]


def weigh(q, keys, held, scale):
    half = keys.shape[0] // 2
    none = jnp.zeros_like(q)
    both = jnp.concatenate([jnp.concatenate([q, none], 1), jnp.concatenate([none, q], 1)], 0)
    lane = lax.broadcasted_iota(jnp.int32, (8, TILE), 1) % 4
    tiles = []
    for j in range(0, half, TILE):
        pair = jnp.concatenate([keys[j : j + TILE, :], keys[half + j : half + j + TILE, :]], 1)
        scores = lax.dot_general(both, pair, (((1,), (1,)), ((), ())), preferred_element_type=jnp.float32)
        for a in (0, 32):
            own = scores[a : a + 8]
            for g in range(1, 4):
                own = jnp.where(lane == g, scores[a + 8 * g : a + 8 * g + 8], own)
            tiles.append(own)
    high = spread(functools.reduce(jnp.maximum, columns(functools.reduce(jnp.maximum, tiles))), jnp.max, -jnp.inf, 4)
    wide = jnp.concatenate([high] * (TILE // 128), 1)
    total = None
    for j in range(half // TILE):
        rows = []
        for own in tiles[2 * j : 2 * j + 2]:
            weights = jnp.exp2((own - wide) * scale)
            total = weights if total is None else total + weights
            rows += [jnp.where(lane == g, weights, 0.0) for g in range(4)]
        held[:, j * TILE : (j + 1) * TILE] = jnp.concatenate(rows, 0).astype(jnp.bfloat16)
    return high, functools.reduce(jnp.add, columns(total))


def gather(held, values):
    half = values.shape[0] // 2
    out = None
    for r in range(0, half, half // 2):
        rows = jnp.concatenate([values[r : r + half // 2, :], values[half + r : half + r + half // 2, :]], 1)
        seen = jnp.dot(held[:, r : r + half // 2], rows, preferred_element_type=jnp.float32)
        seen = seen[0:32, 0:128] + seen[32:64, 128:256]
        out = seen if out is None else out + seen
    return out


def kernel(n, q, k, v, out, qbuf, kbuf, vbuf, held0, held1, high, sums, part, stat, parts, stats, qsem, ksem, vsem, sent, told, handed, came, met, passed, landed):
    me = lax.axis_index("sp")
    mate = me + 1 - 2 * lax.rem(me, 2)
    pairs = q.shape[0] // 2
    units = pairs + 1
    bulk = units - TAIL
    rounds = -(-bulk // n)
    scale = q.shape[2] ** -0.5 * LOG2E
    held = (held0, held1)

    def read(src, buf, sem, slots, i):
        slot = lax.rem(i, slots)
        return pltpu.make_async_copy(src.at[pl.ds(2 * i, 2)], buf.at[slot], sem.at[slot])

    read_k = functools.partial(read, k, kbuf, ksem, K_SLOTS)
    read_v = functools.partial(read, v, vbuf, vsem, V_SLOTS)
    read_q = pltpu.make_async_copy(q, qbuf, qsem)
    read_q.start()
    for i in range(max(K_SLOTS, V_SLOTS)):
        if i < K_SLOTS:
            read_k(i).start()
        if i < V_SLOTS:
            read_v(i).start()

    barrier = pltpu.get_barrier_semaphore()
    for d in range(1, n):
        pl.semaphore_signal(barrier, inc=1, device_id={"sp": lax.rem(me + d, n)}, device_id_type=pl.DeviceIdType.MESH)

    def keys(i, u):
        high[u], sums[u] = weigh(qbuf[2 * i + u], kbuf.at[lax.rem(i, K_SLOTS), u], held[u], scale)

    def values(i, u):
        lane = lax.broadcasted_iota(jnp.int32, (8, 128), 1)
        found = jnp.where(lane % 64 < 32, high[u], spread(sums[u], jnp.sum, 0.0, 4))
        if u == 1:
            stat[i + 1] = found
        else:
            stat[i] = jnp.where(lane < 64, stat[i], found)
        part[i + u, 1 - u] = gather(held[u], vbuf.at[lax.rem(i, V_SLOTS), u]).astype(jnp.bfloat16)

    def few(i):
        return 1 if isinstance(i, int) and i == units - 1 else 2

    def remote(src, dst, send_sem, recv_sem, to):
        return pltpu.make_async_remote_copy(src_ref=src, dst_ref=dst, send_sem=send_sem, recv_sem=recv_sem, device_id={"sp": to}, device_id_type=pl.DeviceIdType.MESH)

    def cut(ref, kind, i):
        return ref.at[pl.ds(0, 1)] if kind == 0 and few(i) == 1 else ref

    def amount(i, kind, count, sem):
        ref = parts.at[0, pl.ds(0, count), pl.ds(0, few(i))] if kind == 0 else stats.at[0, pl.ds(0, count)]
        return remote(ref, ref, sem, sem, mate)

    def send(i, place, to, sems, arrival):
        return [
            remote(cut(src.at[i], kind, i), cut(dst.at[place, me], kind, i), sems.at[kind], arrival.at[kind], to)
            for kind, (src, dst) in enumerate(((part, parts), (stat, stats)))
        ]

    def keep(i, place):
        parts[place, me] = part[i]
        stats[place, me] = stat[i]

    def share(i):
        @pl.when(lax.rem(i, n) == me)
        def _():
            keep(i, i // n)

        @pl.when(lax.rem(i, n) != me)
        def _():
            for copy in send(i, i // n, lax.rem(i, n), sent, came.at[i // n]):
                copy.start()

    def tell(i):
        place = rounds + i - bulk
        for d in range(2, n, 2):
            for copy in send(i, place, lax.rem(me + d, n), told, met.at[i - bulk, 0]):
                copy.start()
        for copy in send(i, place, mate, told, met.at[i - bulk, 1]):
            copy.start()
        keep(i, place)

    def relay(i):
        place = rounds + i - bulk
        for kind, ref in enumerate((parts, stats)):
            amount(i, kind, n // 2 - 1, met.at[i - bulk, 0, kind]).wait_recv()
            for d in range(2, n, 2):
                here = cut(ref.at[place, lax.rem(me + d, n)], kind, i)
                remote(here, here, handed.at[kind], met.at[i - bulk, 1, kind], mate).start()

    def together(i, place, arrival, count):
        for kind in range(2):
            amount(i, kind, count, arrival.at[kind]).wait_recv()
        for u in range(few(i)):
            result = []
            for g in range(4):
                high, total = ([jnp.broadcast_to(stats[place, p][:, at : at + 1], (8, 128)) for p in range(n)] for at in (64 * u + g, 64 * u + 32 + g))
                top = functools.reduce(jnp.maximum, high)
                by = [jnp.exp2((h - top) * scale) for h in high]
                whole = functools.reduce(jnp.add, [w * t for w, t in zip(by, total)])
                seen = functools.reduce(jnp.add, [w * parts[place, p, u, 8 * g : 8 * g + 8, :].astype(jnp.float32) for p, w in enumerate(by)])
                result.append(seen / whole)
            out[2 * i + u] = jnp.concatenate(result, 0).astype(out.dtype)

    def own(i):
        @pl.when((i >= 0) & (i < bulk) & (lax.rem(i + n, n) == me))
        def _():
            together(i, i // n, came.at[i // n], n - 1)
            here = out.at[pl.ds(2 * i, 2)]
            for d in range(1, n):
                remote(here, here, passed, landed, lax.rem(me + d, n)).start()

    read_q.wait()
    read_k(0).wait()
    part[0, 0] = jnp.zeros_like(part[0, 0])
    stat[0] = jnp.ones_like(stat[0])
    keys(0, 0)
    keys(0, 1)
    read_k(K_SLOTS).start()
    read_v(0).wait()
    values(0, 0)
    pl.semaphore_wait(barrier, n - 1)
    share(jnp.int32(0))

    def step(i, _):
        read_k(i).wait()
        read_v(i).wait()
        keys(i, 0)
        values(i - 1, 1)
        keys(i, 1)
        values(i, 0)

        @pl.when(i + K_SLOTS < pairs)
        def _():
            read_k(i + K_SLOTS).start()

        @pl.when(i - 1 + V_SLOTS < pairs)
        def _():
            read_v(i - 1 + V_SLOTS).start()

        @pl.when(i < bulk)
        def _():
            share(i)

        @pl.when(i >= bulk)
        def _():
            tell(i)

        own(i - LAG)
        return 0

    end = pairs - 1
    lax.fori_loop(1, end, step, 0)
    read_k(end).wait()
    keys(end, 0)
    values(end - 1, 1)
    keys(end, 1)
    own(jnp.int32(end - LAG))
    read_v(end).wait()
    values(end, 0)
    tell(end)
    values(end, 1)
    tell(units - 1)

    def rest(i, _):
        own(i)
        return 0

    def sequences(sem, count):
        ref = out.at[pl.ds(0, count)]
        remote(ref, ref, sem, sem, mate).wait_send()

    def settle(mine):
        others = pl.ds(0, bulk - mine)
        remote(part.at[others], part.at[others], sent.at[0], landed, mate).wait()
        remote(stat.at[others], stat.at[others], sent.at[1], landed, mate).wait_send()
        sequences(passed, 2 * mine * (n - 1))

    def finish(i):
        together(i, rounds + i - bulk, met.at[i - bulk, 1], n // 2)

    lax.fori_loop(end + 1 - LAG, bulk, rest, 0)
    for i in range(bulk, units - 2):
        relay(i)
    if units - 2 > bulk:
        finish(bulk)
    relay(units - 2)
    relay(units - 1)
    for i in range(min(bulk + 1, units - 2), units - 1):
        finish(i)
    for sems, copies in ((told, n // 2), (handed, n // 2 - 1)):
        sequences(sems.at[0], copies * (2 * TAIL - 1))
        numbers = stat.at[pl.ds(0, copies * TAIL)]
        remote(numbers, numbers, sems.at[1], sems.at[1], mate).wait_send()
    finish(units - 1)
    more = bulk - (rounds - 1) * n
    pl.when(me < more)(lambda: settle(rounds))
    pl.when(me >= more)(lambda: settle(rounds - 1))


def solution(mesh):
    n = mesh.shape["sp"]

    def step(q, k, v):
        batch, heads, head = q.shape
        units, rows = batch // 2 + 1, k.shape[1] * k.shape[2]
        places = -(-(units - TAIL) // n) + TAIL
        dma = pltpu.SemaphoreType.DMA
        padded = pl.pallas_call(
            functools.partial(kernel, n),
            out_shape=jax.ShapeDtypeStruct((2 * units, heads, head), q.dtype),
            in_specs=[pl.BlockSpec(memory_space=pltpu.HBM)] * 3,
            out_specs=pl.BlockSpec(memory_space=pltpu.VMEM),
            scratch_shapes=[
                pltpu.VMEM(q.shape, q.dtype),
                pltpu.VMEM((K_SLOTS, 2, rows, head), k.dtype),
                pltpu.VMEM((V_SLOTS, 2, rows, head), v.dtype),
                pltpu.VMEM((2 * heads, rows // 2), jnp.bfloat16),
                pltpu.VMEM((2 * heads, rows // 2), jnp.bfloat16),
                pltpu.VMEM((2, 8, 128), jnp.float32),
                pltpu.VMEM((2, 8, 128), jnp.float32),
                pltpu.VMEM((units, 2, heads, head), jnp.bfloat16),
                pltpu.VMEM((units, 8, 128), jnp.float32),
                pltpu.VMEM((places, n, 2, heads, head), jnp.bfloat16),
                pltpu.VMEM((places, n, 8, 128), jnp.float32),
                dma,
                dma((K_SLOTS,)),
                dma((V_SLOTS,)),
                dma((2,)),
                dma((2,)),
                dma((2,)),
                dma((places - TAIL, 2)),
                dma((TAIL, 2, 2)),
                dma,
                dma,
            ],
            compiler_params=pltpu.CompilerParams(collective_id=0, has_side_effects=True, vmem_limit_bytes=48 * 1024 * 1024),
        )(q, k.reshape(batch, rows, head), v.reshape(batch, rows, head))
        return padded[1 : batch + 1]

    return jax.shard_map(
        step,
        mesh=mesh,
        in_specs=(P("dp", None, None), P("dp", "sp", None, None), P("dp", "sp", None, None)),
        out_specs=P("dp", None, None),
        check_vma=False,
    )
```

```python
import functools

import jax
import jax.numpy as jnp
from jax import lax
from jax.experimental import pallas as pl
from jax.experimental.pallas import tpu as pltpu
from jax.sharding import PartitionSpec as P

LOG2E = 1.4426950408889634
TILE = 256
TAIL = 3
LAG = 4
K_SLOTS, V_SLOTS = 4, 5


def spread(x, reduce, fill, kinds):
    lane = lax.broadcasted_iota(jnp.int32, x.shape, 1) % kinds
    out = None
    for g in range(kinds):
        one = jnp.broadcast_to(reduce(jnp.where(lane == g, x, fill), axis=1, keepdims=True), x.shape)
        out = one if out is None else jnp.where(lane == g, one, out)
    return out


def columns(x):
    return [x[:, i : i + 128] for i in range(0, x.shape[1], 128)]


def weigh(q, keys, held, scale):
    half = keys.shape[0] // 2
    none = jnp.zeros_like(q)
    both = jnp.concatenate([jnp.concatenate([q, none], 1), jnp.concatenate([none, q], 1)], 0)
    lane = lax.broadcasted_iota(jnp.int32, (8, TILE), 1) % 4
    tiles = []
    for j in range(0, half, TILE):
        pair = jnp.concatenate([keys[j : j + TILE, :], keys[half + j : half + j + TILE, :]], 1)
        scores = lax.dot_general(both, pair, (((1,), (1,)), ((), ())), preferred_element_type=jnp.float32)
        for a in (0, 32):
            own = scores[a : a + 8]
            for g in range(1, 4):
                own = jnp.where(lane == g, scores[a + 8 * g : a + 8 * g + 8], own)
            tiles.append(own)
    high = spread(functools.reduce(jnp.maximum, columns(functools.reduce(jnp.maximum, tiles))), jnp.max, -jnp.inf, 4)
    wide = jnp.concatenate([high] * (TILE // 128), 1)
    total = None
    for j in range(half // TILE):
        rows = []
        for own in tiles[2 * j : 2 * j + 2]:
            weights = jnp.exp2((own - wide) * scale)
            total = weights if total is None else total + weights
            rows += [jnp.where(lane == g, weights, 0.0) for g in range(4)]
        held[:, j * TILE : (j + 1) * TILE] = jnp.concatenate(rows, 0).astype(jnp.bfloat16)
    return high, functools.reduce(jnp.add, columns(total))


def gather(held, values):
    half = values.shape[0] // 2
    out = None
    for r in range(0, half, half // 2):
        rows = jnp.concatenate([values[r : r + half // 2, :], values[half + r : half + r + half // 2, :]], 1)
        seen = jnp.dot(held[:, r : r + half // 2], rows, preferred_element_type=jnp.float32)
        seen = seen[0:32, 0:128] + seen[32:64, 128:256]
        out = seen if out is None else out + seen
    return out


def kernel(n, q, k, v, out, qbuf, kbuf, vbuf, held0, held1, high, sums, part, stat, parts, stats, qsem, ksem, vsem, sent, told, handed, came, met, passed, landed):
    me = lax.axis_index("sp")
    mate = me + 1 - 2 * lax.rem(me, 2)
    pairs = q.shape[0] // 2
    units = pairs + 1
    bulk = units - TAIL
    rounds = -(-bulk // n)
    scale = q.shape[2] ** -0.5 * LOG2E
    held = (held0, held1)

    def read(src, buf, sem, slots, i):
        slot = lax.rem(i, slots)
        return pltpu.make_async_copy(src.at[pl.ds(2 * i, 2)], buf.at[slot], sem.at[slot])

    read_k = functools.partial(read, k, kbuf, ksem, K_SLOTS)
    read_v = functools.partial(read, v, vbuf, vsem, V_SLOTS)
    read_q = pltpu.make_async_copy(q, qbuf, qsem)
    read_q.start()
    for i in range(max(K_SLOTS, V_SLOTS)):
        if i < K_SLOTS:
            read_k(i).start()
        if i < V_SLOTS:
            read_v(i).start()

    barrier = pltpu.get_barrier_semaphore()
    for d in range(1, n):
        pl.semaphore_signal(barrier, inc=1, device_id={"sp": lax.rem(me + d, n)}, device_id_type=pl.DeviceIdType.MESH)

    def keys(i, u):
        high[u], sums[u] = weigh(qbuf[2 * i + u], kbuf.at[lax.rem(i, K_SLOTS), u], held[u], scale)

    def values(i, u):
        lane = lax.broadcasted_iota(jnp.int32, (8, 128), 1)
        found = jnp.where(lane % 64 < 32, high[u], spread(sums[u], jnp.sum, 0.0, 4))
        if u == 1:
            stat[i + 1] = found
        else:
            stat[i] = jnp.where(lane < 64, stat[i], found)
        part[i + u, 1 - u] = gather(held[u], vbuf.at[lax.rem(i, V_SLOTS), u]).astype(jnp.bfloat16)

    def few(i):
        return 1 if isinstance(i, int) and i == units - 1 else 2

    def remote(src, dst, send_sem, recv_sem, to):
        return pltpu.make_async_remote_copy(src_ref=src, dst_ref=dst, send_sem=send_sem, recv_sem=recv_sem, device_id={"sp": to}, device_id_type=pl.DeviceIdType.MESH)

    def cut(ref, kind, i):
        return ref.at[pl.ds(0, 1)] if kind == 0 and few(i) == 1 else ref

    def amount(i, kind, count, sem):
        ref = parts.at[0, pl.ds(0, count), pl.ds(0, few(i))] if kind == 0 else stats.at[0, pl.ds(0, count)]
        return remote(ref, ref, sem, sem, mate)

    def send(i, place, to, sems, arrival):
        return [
            remote(cut(src.at[i], kind, i), cut(dst.at[place, me], kind, i), sems.at[kind], arrival.at[kind], to)
            for kind, (src, dst) in enumerate(((part, parts), (stat, stats)))
        ]

    def keep(i, place):
        parts[place, me] = part[i]
        stats[place, me] = stat[i]

    def share(i):
        @pl.when(lax.rem(i, n) == me)
        def _():
            keep(i, i // n)

        @pl.when(lax.rem(i, n) != me)
        def _():
            for copy in send(i, i // n, lax.rem(i, n), sent, came.at[i // n]):
                copy.start()

    def tell(i):
        place = rounds + i - bulk
        final = few(i) == 1
        for d in range(1, n) if final else range(2, n, 2):
            for copy in send(i, place, lax.rem(me + d, n), told, met.at[i - bulk, 0]):
                copy.start()
        if not final:
            for copy in send(i, place, mate, told, met.at[i - bulk, 1]):
                copy.start()
        keep(i, place)

    def relay(i):
        place = rounds + i - bulk
        for kind, ref in enumerate((parts, stats)):
            amount(i, kind, n // 2 - 1, met.at[i - bulk, 0, kind]).wait_recv()
            for d in range(2, n, 2):
                here = cut(ref.at[place, lax.rem(me + d, n)], kind, i)
                remote(here, here, handed.at[kind], met.at[i - bulk, 1, kind], mate).start()

    def together(i, place, arrival, count):
        for kind in range(2):
            amount(i, kind, count, arrival.at[kind]).wait_recv()
        for u in range(few(i)):
            result = []
            for g in range(4):
                high, total = ([jnp.broadcast_to(stats[place, p][:, at : at + 1], (8, 128)) for p in range(n)] for at in (64 * u + g, 64 * u + 32 + g))
                top = functools.reduce(jnp.maximum, high)
                by = [jnp.exp2((h - top) * scale) for h in high]
                whole = functools.reduce(jnp.add, [w * t for w, t in zip(by, total)])
                seen = functools.reduce(jnp.add, [w * parts[place, p, u, 8 * g : 8 * g + 8, :].astype(jnp.float32) for p, w in enumerate(by)])
                result.append(seen / whole)
            out[2 * i + u] = jnp.concatenate(result, 0).astype(out.dtype)

    def own(i):
        @pl.when((i >= 0) & (i < bulk) & (lax.rem(i + n, n) == me))
        def _():
            together(i, i // n, came.at[i // n], n - 1)
            here = out.at[pl.ds(2 * i, 2)]
            for d in range(1, n):
                remote(here, here, passed, landed, lax.rem(me + d, n)).start()

    read_q.wait()
    read_k(0).wait()
    part[0, 0] = jnp.zeros_like(part[0, 0])
    stat[0] = jnp.ones_like(stat[0])
    keys(0, 0)
    keys(0, 1)
    read_k(K_SLOTS).start()
    read_v(0).wait()
    values(0, 0)
    pl.semaphore_wait(barrier, n - 1)
    share(jnp.int32(0))

    def step(i, _):
        read_k(i).wait()
        read_v(i).wait()
        keys(i, 0)
        values(i - 1, 1)
        keys(i, 1)
        values(i, 0)

        @pl.when(i + K_SLOTS < pairs)
        def _():
            read_k(i + K_SLOTS).start()

        @pl.when(i - 1 + V_SLOTS < pairs)
        def _():
            read_v(i - 1 + V_SLOTS).start()

        @pl.when(i < bulk)
        def _():
            share(i)

        @pl.when(i >= bulk)
        def _():
            tell(i)

        own(i - LAG)
        return 0

    end = pairs - 1
    lax.fori_loop(1, end, step, 0)
    read_k(end).wait()
    keys(end, 0)
    values(end - 1, 1)
    keys(end, 1)
    own(jnp.int32(end - LAG))
    read_v(end).wait()
    values(end, 0)
    tell(end)
    values(end, 1)
    tell(units - 1)

    def rest(i, _):
        own(i)
        return 0

    def sequences(sem, count):
        ref = out.at[pl.ds(0, count)]
        remote(ref, ref, sem, sem, mate).wait_send()

    def settle(mine):
        others = pl.ds(0, bulk - mine)
        remote(part.at[others], part.at[others], sent.at[0], landed, mate).wait()
        remote(stat.at[others], stat.at[others], sent.at[1], landed, mate).wait_send()
        sequences(passed, 2 * mine * (n - 1))

    def finish(i):
        together(i, rounds + i - bulk, met.at[i - bulk, 1], n // 2)

    lax.fori_loop(end + 1 - LAG, bulk, rest, 0)
    for i in range(bulk, units - 2):
        relay(i)
    if units - 2 > bulk:
        finish(bulk)
    relay(units - 2)
    for i in range(min(bulk + 1, units - 2), units - 1):
        finish(i)
    for sems, copies, more in ((told, n // 2, n - 1), (handed, n // 2 - 1, 0)):
        sequences(sems.at[0], copies * (2 * TAIL - 2) + more)
        numbers = stat.at[pl.ds(0, copies * (TAIL - 1) + more)]
        remote(numbers, numbers, sems.at[1], sems.at[1], mate).wait_send()
    together(units - 1, rounds + TAIL - 1, met.at[TAIL - 1, 0], n - 1)
    more = bulk - (rounds - 1) * n
    pl.when(me < more)(lambda: settle(rounds))
    pl.when(me >= more)(lambda: settle(rounds - 1))


def solution(mesh):
    n = mesh.shape["sp"]

    def step(q, k, v):
        batch, heads, head = q.shape
        units, rows = batch // 2 + 1, k.shape[1] * k.shape[2]
        places = -(-(units - TAIL) // n) + TAIL
        dma = pltpu.SemaphoreType.DMA
        padded = pl.pallas_call(
            functools.partial(kernel, n),
            out_shape=jax.ShapeDtypeStruct((2 * units, heads, head), q.dtype),
            in_specs=[pl.BlockSpec(memory_space=pltpu.HBM)] * 3,
            out_specs=pl.BlockSpec(memory_space=pltpu.VMEM),
            scratch_shapes=[
                pltpu.VMEM(q.shape, q.dtype),
                pltpu.VMEM((K_SLOTS, 2, rows, head), k.dtype),
                pltpu.VMEM((V_SLOTS, 2, rows, head), v.dtype),
                pltpu.VMEM((2 * heads, rows // 2), jnp.bfloat16),
                pltpu.VMEM((2 * heads, rows // 2), jnp.bfloat16),
                pltpu.VMEM((2, 8, 128), jnp.float32),
                pltpu.VMEM((2, 8, 128), jnp.float32),
                pltpu.VMEM((units, 2, heads, head), jnp.bfloat16),
                pltpu.VMEM((units, 8, 128), jnp.float32),
                pltpu.VMEM((places, n, 2, heads, head), jnp.bfloat16),
                pltpu.VMEM((places, n, 8, 128), jnp.float32),
                dma,
                dma((K_SLOTS,)),
                dma((V_SLOTS,)),
                dma((2,)),
                dma((2,)),
                dma((2,)),
                dma((places - TAIL, 2)),
                dma((TAIL, 2, 2)),
                dma,
                dma,
            ],
            compiler_params=pltpu.CompilerParams(collective_id=0, has_side_effects=True, vmem_limit_bytes=48 * 1024 * 1024),
        )(pltpu.with_memory_space_constraint(q, pltpu.HBM), k.reshape(batch, rows, head), v.reshape(batch, rows, head))
        return padded[1 : batch + 1]

    return jax.shard_map(
        step,
        mesh=mesh,
        in_specs=(P("dp", None, None), P("dp", "sp", None, None), P("dp", "sp", None, None)),
        out_specs=P("dp", None, None),
        check_vma=False,
    )
```

```python
import functools

import jax
import jax.numpy as jnp
from jax import lax
from jax.experimental import pallas as pl
from jax.experimental.pallas import tpu as pltpu
from jax.sharding import PartitionSpec as P

LOG2E = 1.4426950408889634
TILE = 256
TAIL = 3
LAG = 4
K_SLOTS, V_SLOTS = 3, 4


def spread(x, reduce, fill, kinds):
    lane = lax.broadcasted_iota(jnp.int32, x.shape, 1) % kinds
    out = None
    for g in range(kinds):
        one = jnp.broadcast_to(reduce(jnp.where(lane == g, x, fill), axis=1, keepdims=True), x.shape)
        out = one if out is None else jnp.where(lane == g, one, out)
    return out


def columns(x):
    return [x[:, i : i + 128] for i in range(0, x.shape[1], 128)]


def weigh(q, keys, held, scale):
    half = keys.shape[0] // 2
    none = jnp.zeros_like(q)
    both = jnp.concatenate([jnp.concatenate([q, none], 1), jnp.concatenate([none, q], 1)], 0)
    lane = lax.broadcasted_iota(jnp.int32, (8, TILE), 1) % 4
    tiles = []
    for j in range(0, half, TILE):
        pair = jnp.concatenate([keys[j : j + TILE, :], keys[half + j : half + j + TILE, :]], 1)
        scores = lax.dot_general(both, pair, (((1,), (1,)), ((), ())), preferred_element_type=jnp.float32)
        for a in (0, 32):
            own = scores[a : a + 8]
            for g in range(1, 4):
                own = jnp.where(lane == g, scores[a + 8 * g : a + 8 * g + 8], own)
            tiles.append(own)
    high = spread(functools.reduce(jnp.maximum, columns(functools.reduce(jnp.maximum, tiles))), jnp.max, -jnp.inf, 4)
    wide = jnp.concatenate([high] * (TILE // 128), 1)
    total = None
    for j in range(half // TILE):
        rows = []
        for own in tiles[2 * j : 2 * j + 2]:
            weights = jnp.exp2((own - wide) * scale)
            total = weights if total is None else total + weights
            rows += [jnp.where(lane == g, weights, 0.0) for g in range(4)]
        held[:, j * TILE : (j + 1) * TILE] = jnp.concatenate(rows, 0).astype(jnp.bfloat16)
    return high, functools.reduce(jnp.add, columns(total))


def gather(held, values):
    half = values.shape[0] // 2
    out = None
    for r in range(0, half, half // 2):
        rows = jnp.concatenate([values[r : r + half // 2, :], values[half + r : half + r + half // 2, :]], 1)
        seen = jnp.dot(held[:, r : r + half // 2], rows, preferred_element_type=jnp.float32)
        seen = seen[0:32, 0:128] + seen[32:64, 128:256]
        out = seen if out is None else out + seen
    return out


def kernel(n, q, k, v, out, qbuf, kbuf, vbuf, held0, held1, high, sums, part, stat, parts, stats, qsem, ksem, vsem, sent, told, handed, came, met, passed, landed):
    me = lax.axis_index("sp")
    mate = me + 1 - 2 * lax.rem(me, 2)
    pairs = q.shape[0] // 2
    units = pairs + 1
    bulk = units - TAIL
    rounds = -(-bulk // n)
    scale = q.shape[2] ** -0.5 * LOG2E
    held = (held0, held1)

    def read(src, buf, sem, slots, i):
        slot = lax.rem(i, slots)
        return pltpu.make_async_copy(src.at[pl.ds(2 * i, 2)], buf.at[slot], sem.at[slot])

    read_k = functools.partial(read, k, kbuf, ksem, K_SLOTS)
    read_v = functools.partial(read, v, vbuf, vsem, V_SLOTS)
    read_q = pltpu.make_async_copy(q, qbuf, qsem)
    read_q.start()
    read_k(0).start()
    read_v(0).start()

    barrier = pltpu.get_barrier_semaphore()
    for d in range(1, n):
        pl.semaphore_signal(barrier, inc=1, device_id={"sp": lax.rem(me + d, n)}, device_id_type=pl.DeviceIdType.MESH)

    def keys(i, u):
        high[u], sums[u] = weigh(qbuf[2 * i + u], kbuf.at[lax.rem(i, K_SLOTS), u], held[u], scale)

    def values(i, u):
        lane = lax.broadcasted_iota(jnp.int32, (8, 128), 1)
        found = jnp.where(lane % 64 < 32, high[u], spread(sums[u], jnp.sum, 0.0, 4))
        if u == 1:
            stat[i + 1] = found
        else:
            stat[i] = jnp.where(lane < 64, stat[i], found)
        part[i + u, 1 - u] = gather(held[u], vbuf.at[lax.rem(i, V_SLOTS), u]).astype(jnp.bfloat16)

    def few(i):
        return 1 if isinstance(i, int) and i == units - 1 else 2

    def remote(src, dst, send_sem, recv_sem, to):
        return pltpu.make_async_remote_copy(src_ref=src, dst_ref=dst, send_sem=send_sem, recv_sem=recv_sem, device_id={"sp": to}, device_id_type=pl.DeviceIdType.MESH)

    def cut(ref, kind, i):
        return ref.at[pl.ds(0, 1)] if kind == 0 and few(i) == 1 else ref

    def amount(i, kind, count, sem):
        ref = parts.at[0, pl.ds(0, count), pl.ds(0, few(i))] if kind == 0 else stats.at[0, pl.ds(0, count)]
        return remote(ref, ref, sem, sem, mate)

    def send(i, place, to, sems, arrival):
        return [
            remote(cut(src.at[i], kind, i), cut(dst.at[place, me], kind, i), sems.at[kind], arrival.at[kind], to)
            for kind, (src, dst) in enumerate(((part, parts), (stat, stats)))
        ]

    def keep(i, place):
        parts[place, me] = part[i]
        stats[place, me] = stat[i]

    def share(i):
        @pl.when(lax.rem(i, n) == me)
        def _():
            keep(i, i // n)

        @pl.when(lax.rem(i, n) != me)
        def _():
            for copy in send(i, i // n, lax.rem(i, n), sent, came.at[i // n]):
                copy.start()

    def tell(i):
        place = rounds + i - bulk
        final = few(i) == 1
        for d in range(1, n) if final else range(2, n, 2):
            for copy in send(i, place, lax.rem(me + d, n), told, met.at[i - bulk, 0]):
                copy.start()
        if not final:
            for copy in send(i, place, mate, told, met.at[i - bulk, 1]):
                copy.start()
        keep(i, place)

    def relay(i):
        place = rounds + i - bulk
        for kind, ref in enumerate((parts, stats)):
            amount(i, kind, n // 2 - 1, met.at[i - bulk, 0, kind]).wait_recv()
            for d in range(2, n, 2):
                here = cut(ref.at[place, lax.rem(me + d, n)], kind, i)
                remote(here, here, handed.at[kind], met.at[i - bulk, 1, kind], mate).start()

    def together(i, place, arrival, count):
        for kind in range(2):
            amount(i, kind, count, arrival.at[kind]).wait_recv()
        for u in range(few(i)):
            result = []
            for g in range(4):
                high, total = ([jnp.broadcast_to(stats[place, p][:, at : at + 1], (8, 128)) for p in range(n)] for at in (64 * u + g, 64 * u + 32 + g))
                top = functools.reduce(jnp.maximum, high)
                by = [jnp.exp2((h - top) * scale) for h in high]
                whole = functools.reduce(jnp.add, [w * t for w, t in zip(by, total)])
                seen = functools.reduce(jnp.add, [w * parts[place, p, u, 8 * g : 8 * g + 8, :].astype(jnp.float32) for p, w in enumerate(by)])
                result.append(seen / whole)
            out[2 * i + u] = jnp.concatenate(result, 0).astype(out.dtype)

    def own(i):
        @pl.when((i >= 0) & (i < bulk) & (lax.rem(i + n, n) == me))
        def _():
            together(i, i // n, came.at[i // n], n - 1)
            here = out.at[pl.ds(2 * i, 2)]
            for d in range(1, n):
                remote(here, here, passed, landed, lax.rem(me + d, n)).start()

    read_q.wait()
    read_k(1).start()
    read_v(1).start()
    read_k(0).wait()
    read_k(2).start()
    read_v(2).start()
    part[0, 0] = jnp.zeros_like(part[0, 0])
    stat[0] = jnp.ones_like(stat[0])
    keys(0, 0)
    keys(0, 1)
    for i in range(3, max(K_SLOTS, V_SLOTS)):
        if i < K_SLOTS:
            read_k(i).start()
        if i < V_SLOTS:
            read_v(i).start()
    read_k(K_SLOTS).start()
    read_v(0).wait()
    values(0, 0)
    pl.semaphore_wait(barrier, n - 1)
    share(jnp.int32(0))

    def step(i, _):
        read_k(i).wait()
        read_v(i).wait()
        keys(i, 0)
        values(i - 1, 1)
        keys(i, 1)
        values(i, 0)

        @pl.when(i + K_SLOTS < pairs)
        def _():
            read_k(i + K_SLOTS).start()

        @pl.when(i - 1 + V_SLOTS < pairs)
        def _():
            read_v(i - 1 + V_SLOTS).start()

        @pl.when(i < bulk)
        def _():
            share(i)

        @pl.when(i >= bulk)
        def _():
            tell(i)

        own(i - LAG)
        return 0

    end = pairs - 1
    lax.fori_loop(1, end, step, 0)
    read_k(end).wait()
    keys(end, 0)
    values(end - 1, 1)
    keys(end, 1)
    own(jnp.int32(end - LAG))
    read_v(end).wait()
    values(end, 0)
    tell(end)
    values(end, 1)
    tell(units - 1)

    def rest(i, _):
        own(i)
        return 0

    def sequences(sem, count):
        ref = out.at[pl.ds(0, count)]
        remote(ref, ref, sem, sem, mate).wait_send()

    def settle(mine):
        others = pl.ds(0, bulk - mine)
        remote(part.at[others], part.at[others], sent.at[0], landed, mate).wait()
        remote(stat.at[others], stat.at[others], sent.at[1], landed, mate).wait_send()
        sequences(passed, 2 * mine * (n - 1))

    def finish(i):
        together(i, rounds + i - bulk, met.at[i - bulk, 1], n // 2)

    lax.fori_loop(end + 1 - LAG, bulk, rest, 0)
    for i in range(bulk, units - 2):
        relay(i)
    if units - 2 > bulk:
        finish(bulk)
    relay(units - 2)
    for i in range(min(bulk + 1, units - 2), units - 1):
        finish(i)
    for sems, copies, more in ((told, n // 2, n - 1), (handed, n // 2 - 1, 0)):
        sequences(sems.at[0], copies * (2 * TAIL - 2) + more)
        numbers = stat.at[pl.ds(0, copies * (TAIL - 1) + more)]
        remote(numbers, numbers, sems.at[1], sems.at[1], mate).wait_send()
    together(units - 1, rounds + TAIL - 1, met.at[TAIL - 1, 0], n - 1)
    more = bulk - (rounds - 1) * n
    pl.when(me < more)(lambda: settle(rounds))
    pl.when(me >= more)(lambda: settle(rounds - 1))


def solution(mesh):
    n = mesh.shape["sp"]

    def step(q, k, v):
        batch, heads, head = q.shape
        units, rows = batch // 2 + 1, k.shape[1] * k.shape[2]
        places = -(-(units - TAIL) // n) + TAIL
        dma = pltpu.SemaphoreType.DMA
        padded = pl.pallas_call(
            functools.partial(kernel, n),
            out_shape=jax.ShapeDtypeStruct((2 * units, heads, head), q.dtype),
            in_specs=[pl.BlockSpec(memory_space=pltpu.HBM)] * 3,
            out_specs=pl.BlockSpec(memory_space=pltpu.VMEM),
            scratch_shapes=[
                pltpu.VMEM(q.shape, q.dtype),
                pltpu.VMEM((K_SLOTS, 2, rows, head), k.dtype),
                pltpu.VMEM((V_SLOTS, 2, rows, head), v.dtype),
                pltpu.VMEM((2 * heads, rows // 2), jnp.bfloat16),
                pltpu.VMEM((2 * heads, rows // 2), jnp.bfloat16),
                pltpu.VMEM((2, 8, 128), jnp.float32),
                pltpu.VMEM((2, 8, 128), jnp.float32),
                pltpu.VMEM((units, 2, heads, head), jnp.bfloat16),
                pltpu.VMEM((units, 8, 128), jnp.float32),
                pltpu.VMEM((places, n, 2, heads, head), jnp.bfloat16),
                pltpu.VMEM((places, n, 8, 128), jnp.float32),
                dma,
                dma((K_SLOTS,)),
                dma((V_SLOTS,)),
                dma((2,)),
                dma((2,)),
                dma((2,)),
                dma((places - TAIL, 2)),
                dma((TAIL, 2, 2)),
                dma,
                dma,
            ],
            compiler_params=pltpu.CompilerParams(collective_id=0, has_side_effects=True, vmem_limit_bytes=48 * 1024 * 1024),
        )(pltpu.with_memory_space_constraint(q, pltpu.HBM), k.reshape(batch, rows, head), v.reshape(batch, rows, head))
        return padded[1 : batch + 1]

    return jax.shard_map(
        step,
        mesh=mesh,
        in_specs=(P("dp", None, None), P("dp", "sp", None, None), P("dp", "sp", None, None)),
        out_specs=P("dp", None, None),
        check_vma=False,
    )
```

```python
import functools

import jax
import jax.numpy as jnp
from jax import lax
from jax.experimental import pallas as pl
from jax.experimental.pallas import tpu as pltpu
from jax.sharding import PartitionSpec as P

LOG2E = 1.4426950408889634
TILE = 256
TAIL = 2
LAG = 4
K_SLOTS, V_SLOTS = 3, 4


def spread(x, reduce, fill, kinds):
    lane = lax.broadcasted_iota(jnp.int32, x.shape, 1) % kinds
    out = None
    for g in range(kinds):
        one = jnp.broadcast_to(reduce(jnp.where(lane == g, x, fill), axis=1, keepdims=True), x.shape)
        out = one if out is None else jnp.where(lane == g, one, out)
    return out


def columns(x):
    return [x[:, i : i + 128] for i in range(0, x.shape[1], 128)]


def weigh(q, keys, held, scale):
    half = keys.shape[0] // 2
    none = jnp.zeros_like(q)
    both = jnp.concatenate([jnp.concatenate([q, none], 1), jnp.concatenate([none, q], 1)], 0)
    lane = lax.broadcasted_iota(jnp.int32, (8, TILE), 1) % 4
    tiles = []
    for j in range(0, half, TILE):
        pair = jnp.concatenate([keys[j : j + TILE, :], keys[half + j : half + j + TILE, :]], 1)
        scores = lax.dot_general(both, pair, (((1,), (1,)), ((), ())), preferred_element_type=jnp.float32)
        for a in (0, 32):
            own = scores[a : a + 8]
            for g in range(1, 4):
                own = jnp.where(lane == g, scores[a + 8 * g : a + 8 * g + 8], own)
            tiles.append(own)
    high = spread(functools.reduce(jnp.maximum, columns(functools.reduce(jnp.maximum, tiles))), jnp.max, -jnp.inf, 4)
    wide = jnp.concatenate([high] * (TILE // 128), 1)
    total = None
    for j in range(half // TILE):
        rows = []
        for own in tiles[2 * j : 2 * j + 2]:
            weights = jnp.exp2((own - wide) * scale)
            total = weights if total is None else total + weights
            rows += [jnp.where(lane == g, weights, 0.0) for g in range(4)]
        held[:, j * TILE : (j + 1) * TILE] = jnp.concatenate(rows, 0).astype(jnp.bfloat16)
    return high, functools.reduce(jnp.add, columns(total))


def gather(held, values):
    half = values.shape[0] // 2
    out = None
    for r in range(0, half, half // 2):
        rows = jnp.concatenate([values[r : r + half // 2, :], values[half + r : half + r + half // 2, :]], 1)
        seen = jnp.dot(held[:, r : r + half // 2], rows, preferred_element_type=jnp.float32)
        seen = seen[0:32, 0:128] + seen[32:64, 128:256]
        out = seen if out is None else out + seen
    return out


def kernel(n, q, k, v, out, qbuf, kbuf, vbuf, held0, held1, high, sums, part, stat, parts, stats, qsem, ksem, vsem, sent, told, handed, came, met, passed, landed):
    me = lax.axis_index("sp")
    mate = me + 1 - 2 * lax.rem(me, 2)
    pairs = q.shape[0] // 2
    units = pairs + 1
    bulk = units - TAIL
    rounds = -(-bulk // n)
    scale = q.shape[2] ** -0.5 * LOG2E
    held = (held0, held1)

    def read(src, buf, sem, slots, i):
        slot = lax.rem(i, slots)
        return pltpu.make_async_copy(src.at[pl.ds(2 * i, 2)], buf.at[slot], sem.at[slot])

    read_k = functools.partial(read, k, kbuf, ksem, K_SLOTS)
    read_v = functools.partial(read, v, vbuf, vsem, V_SLOTS)
    read_q = pltpu.make_async_copy(q, qbuf, qsem)
    read_q.start()
    read_k(0).start()
    read_v(0).start()

    barrier = pltpu.get_barrier_semaphore()
    for d in range(1, n):
        pl.semaphore_signal(barrier, inc=1, device_id={"sp": lax.rem(me + d, n)}, device_id_type=pl.DeviceIdType.MESH)

    def keys(i, u):
        high[u], sums[u] = weigh(qbuf[2 * i + u], kbuf.at[lax.rem(i, K_SLOTS), u], held[u], scale)

    def values(i, u):
        lane = lax.broadcasted_iota(jnp.int32, (8, 128), 1)
        found = jnp.where(lane % 64 < 32, high[u], spread(sums[u], jnp.sum, 0.0, 4))
        if u == 1:
            stat[i + 1] = found
        else:
            stat[i] = jnp.where(lane < 64, stat[i], found)
        part[i + u, 1 - u] = gather(held[u], vbuf.at[lax.rem(i, V_SLOTS), u]).astype(jnp.bfloat16)

    def few(i):
        return 1 if isinstance(i, int) and i == units - 1 else 2

    def remote(src, dst, send_sem, recv_sem, to):
        return pltpu.make_async_remote_copy(src_ref=src, dst_ref=dst, send_sem=send_sem, recv_sem=recv_sem, device_id={"sp": to}, device_id_type=pl.DeviceIdType.MESH)

    def cut(ref, kind, i):
        return ref.at[pl.ds(0, 1)] if kind == 0 and few(i) == 1 else ref

    def amount(i, kind, count, sem):
        ref = parts.at[0, pl.ds(0, count), pl.ds(0, few(i))] if kind == 0 else stats.at[0, pl.ds(0, count)]
        return remote(ref, ref, sem, sem, mate)

    def send(i, place, to, sems, arrival):
        return [
            remote(cut(src.at[i], kind, i), cut(dst.at[place, me], kind, i), sems.at[kind], arrival.at[kind], to)
            for kind, (src, dst) in enumerate(((part, parts), (stat, stats)))
        ]

    def keep(i, place):
        parts[place, me] = part[i]
        stats[place, me] = stat[i]

    def share(i):
        @pl.when(lax.rem(i, n) == me)
        def _():
            keep(i, i // n)

        @pl.when(lax.rem(i, n) != me)
        def _():
            for copy in send(i, i // n, lax.rem(i, n), sent, came.at[i // n]):
                copy.start()

    def tell(i):
        place = rounds + i - bulk
        final = few(i) == 1
        for d in range(1, n) if final else range(2, n, 2):
            for copy in send(i, place, lax.rem(me + d, n), told, met.at[i - bulk, 0]):
                copy.start()
        if not final:
            for copy in send(i, place, mate, told, met.at[i - bulk, 1]):
                copy.start()
        keep(i, place)

    def relay(i):
        place = rounds + i - bulk
        for kind, ref in enumerate((parts, stats)):
            amount(i, kind, n // 2 - 1, met.at[i - bulk, 0, kind]).wait_recv()
            for d in range(2, n, 2):
                here = cut(ref.at[place, lax.rem(me + d, n)], kind, i)
                remote(here, here, handed.at[kind], met.at[i - bulk, 1, kind], mate).start()

    def together(i, place, arrival, count):
        for kind in range(2):
            amount(i, kind, count, arrival.at[kind]).wait_recv()
        for u in range(few(i)):
            result = []
            for g in range(4):
                high, total = ([jnp.broadcast_to(stats[place, p][:, at : at + 1], (8, 128)) for p in range(n)] for at in (64 * u + g, 64 * u + 32 + g))
                top = functools.reduce(jnp.maximum, high)
                by = [jnp.exp2((h - top) * scale) for h in high]
                whole = functools.reduce(jnp.add, [w * t for w, t in zip(by, total)])
                seen = functools.reduce(jnp.add, [w * parts[place, p, u, 8 * g : 8 * g + 8, :].astype(jnp.float32) for p, w in enumerate(by)])
                result.append(seen / whole)
            out[2 * i + u] = jnp.concatenate(result, 0).astype(out.dtype)

    def own(i):
        @pl.when((i >= 0) & (i < bulk) & (lax.rem(i + n, n) == me))
        def _():
            together(i, i // n, came.at[i // n], n - 1)
            here = out.at[pl.ds(2 * i, 2)]
            for d in range(1, n):
                remote(here, here, passed, landed, lax.rem(me + d, n)).start()

    read_q.wait()
    read_k(1).start()
    read_v(1).start()
    read_k(0).wait()
    read_k(2).start()
    read_v(2).start()
    part[0, 0] = jnp.zeros_like(part[0, 0])
    stat[0] = jnp.ones_like(stat[0])
    keys(0, 0)
    keys(0, 1)
    for i in range(3, max(K_SLOTS, V_SLOTS)):
        if i < K_SLOTS:
            read_k(i).start()
        if i < V_SLOTS:
            read_v(i).start()
    read_k(K_SLOTS).start()
    read_v(0).wait()
    values(0, 0)
    pl.semaphore_wait(barrier, n - 1)
    share(jnp.int32(0))

    def step(i, _):
        read_k(i).wait()
        read_v(i).wait()
        keys(i, 0)
        values(i - 1, 1)
        keys(i, 1)
        values(i, 0)

        @pl.when(i + K_SLOTS < pairs)
        def _():
            read_k(i + K_SLOTS).start()

        @pl.when(i - 1 + V_SLOTS < pairs)
        def _():
            read_v(i - 1 + V_SLOTS).start()

        @pl.when(i < bulk)
        def _():
            share(i)

        @pl.when(i >= bulk)
        def _():
            tell(i)

        own(i - LAG)
        return 0

    end = pairs - 1
    lax.fori_loop(1, end, step, 0)
    read_k(end).wait()
    keys(end, 0)
    values(end - 1, 1)
    keys(end, 1)
    own(jnp.int32(end - LAG))
    read_v(end).wait()
    values(end, 0)
    tell(end)
    values(end, 1)
    tell(units - 1)

    def rest(i, _):
        own(i)
        return 0

    def sequences(sem, count):
        ref = out.at[pl.ds(0, count)]
        remote(ref, ref, sem, sem, mate).wait_send()

    def settle(mine):
        others = pl.ds(0, bulk - mine)
        remote(part.at[others], part.at[others], sent.at[0], landed, mate).wait()
        remote(stat.at[others], stat.at[others], sent.at[1], landed, mate).wait_send()
        sequences(passed, 2 * mine * (n - 1))

    def finish(i):
        together(i, rounds + i - bulk, met.at[i - bulk, 1], n // 2)

    lax.fori_loop(end + 1 - LAG, bulk, rest, 0)
    for i in range(bulk, units - 2):
        relay(i)
    if units - 2 > bulk:
        finish(bulk)
    relay(units - 2)
    for i in range(min(bulk + 1, units - 2), units - 1):
        finish(i)
    for sems, copies, more in ((told, n // 2, n - 1), (handed, n // 2 - 1, 0)):
        sequences(sems.at[0], copies * (2 * TAIL - 2) + more)
        numbers = stat.at[pl.ds(0, copies * (TAIL - 1) + more)]
        remote(numbers, numbers, sems.at[1], sems.at[1], mate).wait_send()
    together(units - 1, rounds + TAIL - 1, met.at[TAIL - 1, 0], n - 1)
    more = bulk - (rounds - 1) * n
    pl.when(me < more)(lambda: settle(rounds))
    pl.when(me >= more)(lambda: settle(rounds - 1))


def solution(mesh):
    n = mesh.shape["sp"]

    def step(q, k, v):
        batch, heads, head = q.shape
        units, rows = batch // 2 + 1, k.shape[1] * k.shape[2]
        places = -(-(units - TAIL) // n) + TAIL
        dma = pltpu.SemaphoreType.DMA
        padded = pl.pallas_call(
            functools.partial(kernel, n),
            out_shape=jax.ShapeDtypeStruct((2 * units, heads, head), q.dtype),
            in_specs=[pl.BlockSpec(memory_space=pltpu.HBM)] * 3,
            out_specs=pl.BlockSpec(memory_space=pltpu.VMEM),
            scratch_shapes=[
                pltpu.VMEM(q.shape, q.dtype),
                pltpu.VMEM((K_SLOTS, 2, rows, head), k.dtype),
                pltpu.VMEM((V_SLOTS, 2, rows, head), v.dtype),
                pltpu.VMEM((2 * heads, rows // 2), jnp.bfloat16),
                pltpu.VMEM((2 * heads, rows // 2), jnp.bfloat16),
                pltpu.VMEM((2, 8, 128), jnp.float32),
                pltpu.VMEM((2, 8, 128), jnp.float32),
                pltpu.VMEM((units, 2, heads, head), jnp.bfloat16),
                pltpu.VMEM((units, 8, 128), jnp.float32),
                pltpu.VMEM((places, n, 2, heads, head), jnp.bfloat16),
                pltpu.VMEM((places, n, 8, 128), jnp.float32),
                dma,
                dma((K_SLOTS,)),
                dma((V_SLOTS,)),
                dma((2,)),
                dma((2,)),
                dma((2,)),
                dma((places - TAIL, 2)),
                dma((TAIL, 2, 2)),
                dma,
                dma,
            ],
            compiler_params=pltpu.CompilerParams(collective_id=0, has_side_effects=True, vmem_limit_bytes=48 * 1024 * 1024),
        )(pltpu.with_memory_space_constraint(q, pltpu.HBM), k.reshape(batch, rows, head), v.reshape(batch, rows, head))
        return padded[1 : batch + 1]

    return jax.shard_map(
        step,
        mesh=mesh,
        in_specs=(P("dp", None, None), P("dp", "sp", None, None), P("dp", "sp", None, None)),
        out_specs=P("dp", None, None),
        check_vma=False,
    )
```

```python
import functools

import jax
import jax.numpy as jnp
from jax import lax
from jax.experimental import pallas as pl
from jax.experimental.pallas import tpu as pltpu
from jax.sharding import PartitionSpec as P

LOG2E = 1.4426950408889634
TILE = 256
TAIL = 2
LAG = 4
K_SLOTS, V_SLOTS = 3, 4


def spread(x, reduce, fill, kinds):
    lane = lax.broadcasted_iota(jnp.int32, x.shape, 1) % kinds
    out = None
    for g in range(kinds):
        one = jnp.broadcast_to(reduce(jnp.where(lane == g, x, fill), axis=1, keepdims=True), x.shape)
        out = one if out is None else jnp.where(lane == g, one, out)
    return out


def columns(x):
    return [x[:, i : i + 128] for i in range(0, x.shape[1], 128)]


def weigh(q, keys, held, scale):
    half = keys.shape[0] // 2
    none = jnp.zeros_like(q)
    both = jnp.concatenate([jnp.concatenate([q, none], 1), jnp.concatenate([none, q], 1)], 0)
    lane = lax.broadcasted_iota(jnp.int32, (8, TILE), 1) % 4
    tiles = []
    for j in range(0, half, TILE):
        pair = jnp.concatenate([keys[j : j + TILE, :], keys[half + j : half + j + TILE, :]], 1)
        scores = lax.dot_general(both, pair, (((1,), (1,)), ((), ())), preferred_element_type=jnp.float32)
        for a in (0, 32):
            own = scores[a : a + 8]
            for g in range(1, 4):
                own = jnp.where(lane == g, scores[a + 8 * g : a + 8 * g + 8], own)
            tiles.append(own)
    high = spread(functools.reduce(jnp.maximum, columns(functools.reduce(jnp.maximum, tiles))), jnp.max, -jnp.inf, 4)
    wide = jnp.concatenate([high] * (TILE // 128), 1)
    total = None
    for j in range(half // TILE):
        rows = []
        for own in tiles[2 * j : 2 * j + 2]:
            weights = jnp.exp2((own - wide) * scale)
            total = weights if total is None else total + weights
            rows += [jnp.where(lane == g, weights, 0.0) for g in range(4)]
        held[:, j * TILE : (j + 1) * TILE] = jnp.concatenate(rows, 0).astype(jnp.bfloat16)
    return high, functools.reduce(jnp.add, columns(total))


def gather(held, values):
    half = values.shape[0] // 2
    out = None
    for r in range(0, half, half // 2):
        rows = jnp.concatenate([values[r : r + half // 2, :], values[half + r : half + r + half // 2, :]], 1)
        seen = jnp.dot(held[:, r : r + half // 2], rows, preferred_element_type=jnp.float32)
        seen = seen[0:32, 0:128] + seen[32:64, 128:256]
        out = seen if out is None else out + seen
    return out


def kernel(n, q, k, v, out, qbuf, kbuf, vbuf, held0, held1, high, sums, part, stat, parts, stats, qsem, ksem, vsem, sent, told, handed, came, met, passed, landed):
    me = lax.axis_index("sp")
    mate = me + 1 - 2 * lax.rem(me, 2)
    pairs = q.shape[0] // 2
    units = pairs + 1
    bulk = units - TAIL
    rounds = -(-bulk // n)
    scale = q.shape[2] ** -0.5 * LOG2E
    held = (held0, held1)

    def read(src, buf, sem, slots, i):
        slot = lax.rem(i, slots)
        return pltpu.make_async_copy(src.at[pl.ds(2 * i, 2)], buf.at[slot], sem.at[slot])

    read_k = functools.partial(read, k, kbuf, ksem, K_SLOTS)
    read_v = functools.partial(read, v, vbuf, vsem, V_SLOTS)
    read_q = pltpu.make_async_copy(q, qbuf, qsem)
    read_q.start()
    read_k(0).start()
    read_v(0).start()

    barrier = pltpu.get_barrier_semaphore()
    for d in range(1, n):
        pl.semaphore_signal(barrier, inc=1, device_id={"sp": lax.rem(me + d, n)}, device_id_type=pl.DeviceIdType.MESH)

    def keys(i, u):
        high[u], sums[u] = weigh(qbuf[2 * i + u], kbuf.at[lax.rem(i, K_SLOTS), u], held[u], scale)

    def values(i, u):
        lane = lax.broadcasted_iota(jnp.int32, (8, 128), 1)
        found = jnp.where(lane % 64 < 32, high[u], spread(sums[u], jnp.sum, 0.0, 4))
        if u == 1:
            stat[i + 1] = found
        else:
            stat[i] = jnp.where(lane < 64, stat[i], found)
        part[i + u, 1 - u] = gather(held[u], vbuf.at[lax.rem(i, V_SLOTS), u]).astype(jnp.bfloat16)

    def few(i):
        return 1 if isinstance(i, int) and i == units - 1 else 2

    def remote(src, dst, send_sem, recv_sem, to):
        return pltpu.make_async_remote_copy(src_ref=src, dst_ref=dst, send_sem=send_sem, recv_sem=recv_sem, device_id={"sp": to}, device_id_type=pl.DeviceIdType.MESH)

    def cut(ref, kind, i):
        return ref.at[pl.ds(0, 1)] if kind == 0 and few(i) == 1 else ref

    def amount(i, kind, count, sem):
        ref = parts.at[0, pl.ds(0, count), pl.ds(0, few(i))] if kind == 0 else stats.at[0, pl.ds(0, count)]
        return remote(ref, ref, sem, sem, mate)

    def send(i, place, to, sems, arrival):
        return [
            remote(cut(src.at[i], kind, i), cut(dst.at[place, me], kind, i), sems.at[kind], arrival.at[kind], to)
            for kind, (src, dst) in enumerate(((part, parts), (stat, stats)))
        ]

    def keep(i, place):
        parts[place, me] = part[i]
        stats[place, me] = stat[i]

    def share(i):
        @pl.when(lax.rem(i, n) == me)
        def _():
            keep(i, i // n)

        @pl.when(lax.rem(i, n) != me)
        def _():
            for copy in send(i, i // n, lax.rem(i, n), sent, came.at[i // n]):
                copy.start()

    def tell(i):
        place = rounds + i - bulk
        final = few(i) == 1
        for d in range(1, n) if final else range(2, n, 2):
            for copy in send(i, place, lax.rem(me + d, n), told, met.at[i - bulk, 0]):
                copy.start()
        if not final:
            for copy in send(i, place, mate, told, met.at[i - bulk, 1]):
                copy.start()
        keep(i, place)

    def relay(i):
        place = rounds + i - bulk
        for kind, ref in enumerate((parts, stats)):
            amount(i, kind, n // 2 - 1, met.at[i - bulk, 0, kind]).wait_recv()
            for d in range(2, n, 2):
                here = cut(ref.at[place, lax.rem(me + d, n)], kind, i)
                remote(here, here, handed.at[kind], met.at[i - bulk, 1, kind], mate).start()

    def together(i, place, arrival, count):
        for kind in range(2):
            amount(i, kind, count, arrival.at[kind]).wait_recv()
        for u in range(few(i)):
            result = []
            for g in range(4):
                high, total = ([jnp.broadcast_to(stats[place, p][:, at : at + 1], (8, 128)) for p in range(n)] for at in (64 * u + g, 64 * u + 32 + g))
                top = functools.reduce(jnp.maximum, high)
                by = [jnp.exp2((h - top) * scale) for h in high]
                whole = functools.reduce(jnp.add, [w * t for w, t in zip(by, total)])
                seen = functools.reduce(jnp.add, [w * parts[place, p, u, 8 * g : 8 * g + 8, :].astype(jnp.float32) for p, w in enumerate(by)])
                result.append(seen / whole)
            out[2 * i + u] = jnp.concatenate(result, 0).astype(out.dtype)

    def own(i):
        @pl.when((i >= 0) & (i < bulk) & (lax.rem(i + n, n) == me))
        def _():
            together(i, i // n, came.at[i // n], n - 1)
            here = out.at[pl.ds(2 * i, 2)]
            for d in range(1, n):
                remote(here, here, passed, landed, lax.rem(me + d, n)).start()

    read_q.wait()
    read_k(1).start()
    read_v(1).start()
    read_k(0).wait()
    read_k(2).start()
    read_v(2).start()
    part[0, 0] = jnp.zeros_like(part[0, 0])
    stat[0] = jnp.ones_like(stat[0])
    keys(0, 0)
    keys(0, 1)
    for i in range(3, max(K_SLOTS, V_SLOTS)):
        if i < K_SLOTS:
            read_k(i).start()
        if i < V_SLOTS:
            read_v(i).start()
    read_k(K_SLOTS).start()
    read_v(0).wait()
    values(0, 0)
    pl.semaphore_wait(barrier, n - 1)
    share(jnp.int32(0))

    def step(i, _):
        read_k(i).wait()
        read_v(i).wait()
        keys(i, 0)
        values(i - 1, 1)
        keys(i, 1)
        pl.when(i + K_SLOTS < pairs)(lambda: read_k(i + K_SLOTS).start())
        pl.when(i - 1 + V_SLOTS < pairs)(lambda: read_v(i - 1 + V_SLOTS).start())
        values(i, 0)

        @pl.when(i < bulk)
        def _():
            share(i)

        @pl.when(i >= bulk)
        def _():
            tell(i)

        own(i - LAG)
        return 0

    end = pairs - 1
    lax.fori_loop(1, end, step, 0)
    read_k(end).wait()
    keys(end, 0)
    values(end - 1, 1)
    keys(end, 1)
    own(jnp.int32(end - LAG))
    read_v(end).wait()
    values(end, 0)
    tell(end)
    values(end, 1)
    tell(units - 1)

    def rest(i, _):
        own(i)
        return 0

    def sequences(sem, count):
        ref = out.at[pl.ds(0, count)]
        remote(ref, ref, sem, sem, mate).wait_send()

    def settle(mine):
        others = pl.ds(0, bulk - mine)
        remote(part.at[others], part.at[others], sent.at[0], landed, mate).wait()
        remote(stat.at[others], stat.at[others], sent.at[1], landed, mate).wait_send()
        sequences(passed, 2 * mine * (n - 1))

    def finish(i):
        together(i, rounds + i - bulk, met.at[i - bulk, 1], n // 2)

    lax.fori_loop(end + 1 - LAG, bulk, rest, 0)
    for i in range(bulk, units - 2):
        relay(i)
    if units - 2 > bulk:
        finish(bulk)
    relay(units - 2)
    for i in range(min(bulk + 1, units - 2), units - 1):
        finish(i)
    for sems, copies, more in ((told, n // 2, n - 1), (handed, n // 2 - 1, 0)):
        sequences(sems.at[0], copies * (2 * TAIL - 2) + more)
        numbers = stat.at[pl.ds(0, copies * (TAIL - 1) + more)]
        remote(numbers, numbers, sems.at[1], sems.at[1], mate).wait_send()
    together(units - 1, rounds + TAIL - 1, met.at[TAIL - 1, 0], n - 1)
    more = bulk - (rounds - 1) * n
    pl.when(me < more)(lambda: settle(rounds))
    pl.when(me >= more)(lambda: settle(rounds - 1))


def solution(mesh):
    n = mesh.shape["sp"]

    def step(q, k, v):
        batch, heads, head = q.shape
        units, rows = batch // 2 + 1, k.shape[1] * k.shape[2]
        places = -(-(units - TAIL) // n) + TAIL
        dma = pltpu.SemaphoreType.DMA
        padded = pl.pallas_call(
            functools.partial(kernel, n),
            out_shape=jax.ShapeDtypeStruct((2 * units, heads, head), q.dtype),
            in_specs=[pl.BlockSpec(memory_space=pltpu.HBM)] * 3,
            out_specs=pl.BlockSpec(memory_space=pltpu.VMEM),
            scratch_shapes=[
                pltpu.VMEM(q.shape, q.dtype),
                pltpu.VMEM((K_SLOTS, 2, rows, head), k.dtype),
                pltpu.VMEM((V_SLOTS, 2, rows, head), v.dtype),
                pltpu.VMEM((2 * heads, rows // 2), jnp.bfloat16),
                pltpu.VMEM((2 * heads, rows // 2), jnp.bfloat16),
                pltpu.VMEM((2, 8, 128), jnp.float32),
                pltpu.VMEM((2, 8, 128), jnp.float32),
                pltpu.VMEM((units, 2, heads, head), jnp.bfloat16),
                pltpu.VMEM((units, 8, 128), jnp.float32),
                pltpu.VMEM((places, n, 2, heads, head), jnp.bfloat16),
                pltpu.VMEM((places, n, 8, 128), jnp.float32),
                dma,
                dma((K_SLOTS,)),
                dma((V_SLOTS,)),
                dma((2,)),
                dma((2,)),
                dma((2,)),
                dma((places - TAIL, 2)),
                dma((TAIL, 2, 2)),
                dma,
                dma,
            ],
            compiler_params=pltpu.CompilerParams(collective_id=0, has_side_effects=True, vmem_limit_bytes=48 * 1024 * 1024),
        )(pltpu.with_memory_space_constraint(q, pltpu.HBM), k.reshape(batch, rows, head), v.reshape(batch, rows, head))
        return padded[1 : batch + 1]

    return jax.shard_map(
        step,
        mesh=mesh,
        in_specs=(P("dp", None, None), P("dp", "sp", None, None), P("dp", "sp", None, None)),
        out_specs=P("dp", None, None),
        check_vma=False,
    )
```
